32 devices in a mesh: beam: 8 (over z, y), mp: 4 (over x, core).
Axes of the slice: x: 2, y: 2, z: 4, core: 2. Of those that a mesh axis runs over, the one named last changes fastest.
Arguments:
- token_ids: int32 [512], P('beam'), may hold values from 0 to 128255
- parents: int32 [64, 8, 1], P('beam'), may hold values from 0 to 7; in each aligned block of 512 rows (0 to 511, 512 to 1023, ..., all dimensions but the last counted through in order) at most 192 rows name the same one
- embedding: bfloat16 [128256, 8192], P('mp', 'beam'), may hold values from -6 to 6
- norm_gain: bfloat16 [8192], P('beam'), may hold values from 0.099609375 to 1.8984375
- query_weight: bfloat16 [8192, 8192], P('beam', 'mp'), may hold values from -0.0625 to 0.0625
- key_weight: bfloat16 [8192, 1024], P('beam', 'mp'), may hold values from -0.0625 to 0.0625
- value_weight: bfloat16 [8192, 1024], P('beam', 'mp'), may hold values from -0.0625 to 0.0625
- output_weight: bfloat16 [8192, 8192], P('mp', 'beam'), may hold values from -0.0625 to 0.0625
- cache_keys: bfloat16 [512, 512, 1024], P('beam', None, 'mp'), may hold values from -30 to 30
- cache_values: bfloat16 [512, 512, 1024], P('beam', None, 'mp'), may hold values from -32 to 32
Outputs:
- attention_out: bfloat16 [512, 8192], P('mp', 'beam')
- new_keys: bfloat16 [512, 1024], P('beam', 'mp')
- new_values: bfloat16 [512, 1024], P('beam', 'mp')
The draws below stay inside these ranges and needn't reach their ends.
Inputs may be any that keep to these rules, and one draw needn't show every extreme that they name: parents lie in 0 to 7. Split the requests into aligned blocks of 64 requests; among the new beams of one block, no parent index is named more than 192 times, and in some blocks one is named exactly 192 times.
All inputs are finite; a program needn't handle non-finite values.
Results may differ from the reference program's by a relative error of at most 0.0071.
The reference program's roundings to bfloat16 on the way (of `embedded`, `scaled`, `weights` and `attended`) count: a program that leaves them out, or rounds other values in their place, can miss the bound.
Values may be sent and summed in bfloat16 or wider, within the bound.
No kernel may reach another device: no remote copies, remote signals or barrier semaphores. Data moves between devices by JAX's collectives and lax.ppermute only.
A program may use at most 320 MiB of HBM per device.

```python
import math
import jax
import jax.numpy as jnp
import numpy as np
from jax import lax

D = 8192
HEADS = 64
KV_HEADS = 8
HEAD_DIM = 128
VOCAB = 128256
LEN = 512
REQS = 64
BEAMS = 8
ROWS = 512
ROWS_DEV = 64
CAP = 192


def draw_cache_keys(key, part):
    normals = jax.random.normal(key, (ROWS, LEN, KV_HEADS * HEAD_DIM), jnp.float32) * 1.5
    return jnp.clip(normals, -30.0, 30.0).astype(jnp.bfloat16)


def touch_ends(values, own_key, least, top_value):
    index_at = [jax.random.randint(jax.random.fold_in(own_key, axis), (), 0, length) for axis, length in enumerate(values.shape)]
    longest = values.shape.index(max(values.shape))
    beside = index_at[:longest] + [(index_at[longest] + 1) % values.shape[longest]] + index_at[longest + 1:]
    return values.at[tuple(index_at)].set(least).at[tuple(beside)].set(top_value)


def raised(entries, key, source, target, blocks, factor):
    owner, partner = [(jnp.arange(entries.shape[axis_at]) // (entries.shape[axis_at] // blocks)).reshape([-1 if axis == axis_at else 1 for axis in range(entries.ndim)]) for axis_at in (source, target)]
    chosen = jax.random.permutation(key, blocks)[partner]
    strong = (owner == chosen) | (owner == (partner + blocks // 2) % blocks)
    return jnp.where(strong, factor * entries, entries)


def shard_levels(key, dims, cuts, low, high):
    level = 1.0
    for axis_at, shards_of in cuts:
        heights = jax.random.uniform(jax.random.fold_in(jax.random.fold_in(key, 6), axis_at), (shards_of,), jnp.float32, low / len(cuts), high / len(cuts))
        level = level * jnp.repeat(jnp.exp(heights), dims[axis_at] // shards_of).reshape((-1,) + (1,) * (len(dims) - 1 - axis_at))
    return level


def skewed_wide(rng, dims, number_of, lean):
    loads = [min(1 << octave, number_of + 1 - (1 << octave)) * (1 << 20) // math.isqrt((1 << octave) ** lean) + 1 for octave in range((number_of + 1).bit_length()) if 1 << octave <= number_of]
    scale = 1 + sum(loads) // (1 << 30)
    listing = np.cumsum(np.array([max(1, weight // scale) for weight in loads]))
    ticket = jax.random.randint(jax.random.fold_in(rng, 1), dims, 0, int(listing[len(loads) - 1]))
    start = jnp.left_shift(1, jnp.searchsorted(jnp.asarray(listing, jnp.int32), ticket, side="right").astype(jnp.int32))
    rank = start - 1 + jax.random.randint(jax.random.fold_in(rng, 4), dims, 0, 1 << 30) % jnp.minimum(start, number_of + 1 - start)
    return jax.random.permutation(jax.random.fold_in(rng, 2), number_of)[rank].astype(jnp.int32)


def routed_block(own_key, own, number, rows, count, top, most, skew):
    ranking = jax.random.permutation(own_key, count)
    heavy_load, usual = portions_of(count, rows * top, most, skew, True), portions_of(count, rows * top, most, skew, False)
    places = jnp.arange(count)

    def named(tallies, turn):
        used = int((tallies > 0).sum())
        fixed = max(1, used // 4)
        passed = fixed + (places - fixed + turn * (used - fixed)) % max(1, count - fixed)
        return jnp.zeros((count,), jnp.int32).at[ranking[jnp.where(places < fixed, places, passed)]].set(jnp.asarray(tallies, jnp.int32))

    tallies = jnp.where(number % 4 == 0, named(heavy_load, number // 4), named(usual, number - number // 4 - 1))
    mixed = jax.random.permutation(jax.random.fold_in(own, 3), count)
    source_of, taker = mixed[0:count // 2 * 2:2], mixed[1:count // 2 * 2:2]
    margin = jnp.minimum(tallies[source_of] - 1, most - tallies[taker]) // 2
    margin = jnp.where((source_of == ranking[0]) | (taker == ranking[0]) | (tallies[taker] == 0), 0, jnp.maximum(margin, 0))
    passed = jax.random.randint(jax.random.fold_in(own, 4), (count // 2,), 0, 1 << 20) % (margin + 1)
    tallies = tallies.at[source_of].add(-passed).at[taker].add(passed)
    labels = jnp.searchsorted(jnp.cumsum(tallies), jnp.arange(rows * top), side="right").astype(jnp.int32)
    table = labels.reshape(top, rows).T
    table = table[jax.random.permutation(jax.random.fold_in(own, 1), rows)]
    turn = jax.random.randint(jax.random.fold_in(own, 2), (rows, 1), 0, top)
    return jnp.take_along_axis(table, (jnp.arange(top)[None, :] + turn) % top, axis=1)


def portions_of(count, total, limit, lean, full):
    weights = [(1 << 20) // math.isqrt(grade ** lean) + 1 for grade in range(1, count + 1)]
    largest = limit if full else min(limit, max(-(-total // count), total * weights[0] // sum(weights)))
    least = 1 if total - largest >= count - 1 else 0
    given, rest = [largest] + [least] * (count - 1), total - largest - least * (count - 1)
    while rest > 0:
        candidates = [i for i in range(1, count) if given[i] < largest] or [i for i in range(1, count) if given[i] < limit]
        pool, left = sum([weights[i] for i in candidates]), rest
        for i in candidates:
            extra = min(limit - given[i], max(1, left * weights[i] // pool), rest)
            given[i] = given[i] + extra
            rest = rest - extra
    return np.array(given)


def normal_values(own_key, shape, deviation, limit, shards=(), held_as=jnp.bfloat16):
    gain = shard_levels(own_key, shape, shards, -0.22, 0.18) if shards else 1.0
    array = jax.random.normal(own_key, shape, jnp.float32) * deviation * gain
    return jnp.minimum(jnp.maximum(array, -limit), limit).astype(held_as)


def heavy_noise(key, shape, width, bound, shards, heavy, kind=jnp.bfloat16):
    result = width * jax.random.normal(key, shape, jnp.float32)
    if shards:
        result = result * shard_levels(key, shape, shards, -0.22, 0.18)
    return jnp.clip(raised(result, jax.random.fold_in(key, 3), *heavy), -bound, bound).astype(kind)


def setup_inputs(seed: int = 0) -> dict:
    key_list = jax.random.split(jax.random.key(seed), 11)
    token_ids = touch_ends(skewed_wide(key_list[0], (ROWS,), VOCAB, 2), jax.random.fold_in(key_list[0], 3), 0, VOCAB - 1).astype(jnp.int32)
    parents_keys = jax.random.split(jax.random.fold_in(key_list[1], 1), REQS * BEAMS // (ROWS_DEV * BEAMS))
    parents_turns = jax.random.permutation(jax.random.fold_in(key_list[1], 3), REQS * BEAMS // (ROWS_DEV * BEAMS))
    parents = jax.vmap(lambda own, number: routed_block(jax.random.fold_in(key_list[1], 2), own, number, ROWS_DEV * BEAMS, BEAMS, 1, CAP, 2))(parents_keys, parents_turns).reshape((REQS, BEAMS, 1))
    embedding = heavy_noise(key_list[2], (VOCAB, D), 1.0, 6.0, ((0, 4), (1, 8)), (1, 0, 8, 2.0))
    norm_gain = jnp.clip(1.0 + 0.18 * jax.random.normal(key_list[3], (D,), jnp.float32), 0.099609375, 1.8984375).astype(jnp.bfloat16)
    query_weight = normal_values(key_list[4], (D, HEADS * HEAD_DIM), D ** -0.5, 0.0625, ((0, 8), (1, 4)))
    key_weight = normal_values(key_list[5], (D, KV_HEADS * HEAD_DIM), D ** -0.5, 0.0625, ((0, 8), (1, 4)))
    value_weight = normal_values(key_list[6], (D, KV_HEADS * HEAD_DIM), D ** -0.5, 0.0625, ((0, 8), (1, 4)))
    output_weight = normal_values(key_list[7], (HEADS * HEAD_DIM, D), (HEADS * HEAD_DIM) ** -0.5, 0.0625, ((0, 4), (1, 8)))
    cache_keys = draw_cache_keys(jax.random.fold_in(key_list[10], 71), 0)
    cache_values = normal_values(key_list[9], (ROWS, LEN, KV_HEADS * HEAD_DIM), 4.0, 32.0, ((0, 8), (2, 4)))
    return {"token_ids": token_ids, "parents": parents, "embedding": embedding, "norm_gain": norm_gain, "query_weight": query_weight, "key_weight": key_weight, "value_weight": value_weight, "output_weight": output_weight, "cache_keys": cache_keys, "cache_values": cache_values}


epsilon = 1e-05
rope_base = 500000.0

def apply_rotary(tensor):
    half_dim = HEAD_DIM // 2
    frequency = rope_base ** (-(jnp.arange(half_dim, dtype=jnp.float32) * 2.0 / HEAD_DIM))
    angles = LEN * frequency
    cosine_table = jnp.cos(angles)
    sine_part = jnp.sin(angles)
    front_half = tensor[..., :half_dim]
    back_half = tensor[..., half_dim:]
    return jnp.concatenate([front_half * cosine_table - back_half * sine_part, back_half * cosine_table + front_half * sine_part], axis=-1)

def reference(token_ids, parents, embedding, norm_gain, query_weight, key_weight, value_weight, output_weight, cache_keys, cache_values):
    row_count = BEAMS * REQS
    embedded = embedding[token_ids]
    widened = embedded.astype(jnp.float32)
    mean_square = lax.optimization_barrier(jnp.mean(widened * widened, axis=1, keepdims=True))
    inverse = 1.0 / jnp.sqrt(mean_square + epsilon)
    scaled = (widened * norm_gain.astype(jnp.float32)[None, :]).astype(jnp.bfloat16)
    query_portion = jnp.dot(scaled, query_weight, preferred_element_type=jnp.float32)
    key_part = jnp.dot(scaled, key_weight, preferred_element_type=jnp.float32)
    value_part = jnp.dot(scaled, value_weight, preferred_element_type=jnp.float32)
    query_matrix = apply_rotary((query_portion * inverse).reshape(row_count, HEADS, HEAD_DIM)).astype(jnp.bfloat16)
    new_keys = apply_rotary((key_part * inverse).reshape(row_count, KV_HEADS, HEAD_DIM)).astype(jnp.bfloat16)
    new_values = (value_part * inverse).astype(jnp.bfloat16).reshape(row_count, KV_HEADS, HEAD_DIM)
    parent_rows = (jnp.transpose(parents[:, :, 0]).astype(jnp.int32) * REQS + jnp.arange(REQS, dtype=jnp.int32)[None, :]).reshape(row_count).astype(jnp.int32)
    groups = HEADS // KV_HEADS
    keys_by_head = cache_keys.reshape(row_count, LEN, KV_HEADS, HEAD_DIM)
    values_by_head = cache_values.reshape(row_count, LEN, KV_HEADS, HEAD_DIM)
    scale_factor = HEAD_DIM ** (-0.5)

    def one_head(head_index):
        head_index = head_index.astype(jnp.int32)
        head_keys = lax.dynamic_index_in_dim(keys_by_head, head_index, axis=2, keepdims=False)[parent_rows].astype(jnp.float32)
        head_values = lax.dynamic_index_in_dim(values_by_head, head_index, axis=2, keepdims=False)[parent_rows].astype(jnp.float32)
        head_queries = lax.dynamic_slice_in_dim(query_matrix, head_index * groups, groups, axis=1).astype(jnp.float32)
        fresh_key = lax.dynamic_index_in_dim(new_keys, head_index, axis=1, keepdims=False).astype(jnp.float32)
        fresh_value = lax.dynamic_index_in_dim(new_values, head_index, axis=1, keepdims=False).astype(jnp.float32)
        scores = jnp.einsum('rgd,rld->rgl', head_queries, head_keys) * scale_factor
        own_score = jnp.einsum('rgd,rd->rg', head_queries, fresh_key) * scale_factor
        ceiling = jnp.maximum(lax.optimization_barrier(jnp.max(scores, axis=-1)), own_score)
        weights = jnp.exp(scores - ceiling[..., None])
        own_weight = jnp.exp(own_score - ceiling)
        softmax_divisor = lax.optimization_barrier(jnp.sum(weights, axis=-1)) + own_weight
        attention_weights = lax.optimization_barrier((weights / softmax_divisor[..., None]).astype(jnp.bfloat16)).astype(jnp.float32)
        own_share = lax.optimization_barrier((own_weight / softmax_divisor).astype(jnp.bfloat16)).astype(jnp.float32)
        mixture = jnp.einsum('rgl,rld->rgd', attention_weights, head_values) + own_share[..., None] * fresh_value[:, None, :]
        return mixture.astype(jnp.bfloat16)
    per_head = lax.map(one_head, jnp.arange(KV_HEADS, dtype=jnp.int32))
    attended = jnp.transpose(per_head, (1, 0, 2, 3)).reshape(row_count, HEADS * HEAD_DIM)
    attention_out = jnp.dot(attended, output_weight, preferred_element_type=jnp.float32).astype(jnp.bfloat16)
    return (attention_out, new_keys.reshape(row_count, KV_HEADS * HEAD_DIM), new_values.reshape(row_count, KV_HEADS * HEAD_DIM))
```

```python
import functools

import jax
import jax.numpy as jnp
import numpy as np
from jax import lax
from jax.experimental import pallas as pl
from jax.experimental.pallas import tpu as pltpu
from jax.sharding import PartitionSpec as P

HEAD_DIM = 128
LANES = 128
TILE = 8
LIFT = 8.0
SHRINK = 64.0
VISIT_MIB = 12
epsilon = 1e-05
rope_base = 500000.0


f32 = jnp.float32
bf16 = jnp.bfloat16
f16 = jnp.float16
VMEM = pl.BlockSpec(memory_space=pltpu.VMEM)


def params(mib=48, **more):
    return pltpu.CompilerParams(vmem_limit_bytes=mib << 20, **more)


def cycle(count):
    width = 1 << ((count.bit_length() - 1) // 2)
    height = count // width
    if width == 1 or height % 2:
        return list(range(count))
    walk = []
    for z in range(height):
        ys = range(1, width) if z % 2 == 0 else range(width - 1, 0, -1)
        walk += [z * width + y for y in ys]
    return walk + [z * width for z in range(height - 1, -1, -1)]


def lookup_kernel(group, block_ref, pick_ref, table_ref, out_ref, held, sems):
    rows = out_ref.shape[0]
    groups = rows // group
    held[...] = jnp.zeros_like(held)

    def copy(i, g):
        source = pl.multiple_of(jnp.maximum(block_ref[i], 0) * TILE, TILE)
        target = pl.multiple_of(i * TILE, TILE)
        return pltpu.make_async_copy(
            table_ref.at[pl.ds(source, TILE), :], held.at[pl.ds(target, TILE), :], sems.at[g]
        )

    def issue(g, _):
        for n in range(group):
            i = g * group + n

            @pl.when(block_ref[i] >= 0)
            def _():
                copy(i, g).start()

        return 0

    lax.fori_loop(0, groups, issue, 0)

    def pick(g, _):
        for n in range(group):
            i = g * group + n

            @pl.when(block_ref[i] >= 0)
            def _():
                copy(i, g).wait()

        span = pl.ds(pl.multiple_of(g * group * TILE, group * TILE), group * TILE)
        own = pl.ds(pl.multiple_of(g * group, group), group)
        wanted = pick_ref[own, :]
        column = lax.broadcasted_iota(jnp.int32, (group, group * TILE), 1)
        row = lax.broadcasted_iota(jnp.int32, (group, group * TILE), 0)
        chosen = (column - row * TILE == wanted).astype(f32).astype(bf16)
        out_ref[own, :] = jnp.dot(chosen, held[span, :], preferred_element_type=f32).astype(bf16)
        return 0

    lax.fori_loop(0, groups, pick, 0)


def lookup(ids, table):
    rows, (vocab, width) = ids.shape[0], table.shape
    local = ids - lax.axis_index("mp") * vocab
    inside = (local >= 0) & (local < vocab)
    block = jnp.where(inside, local // TILE, -1)
    pick = jnp.where(inside, local % TILE, rows * TILE)[:, None]
    group = 32
    return pl.pallas_call(
        functools.partial(lookup_kernel, group),
        grid_spec=pltpu.PrefetchScalarGridSpec(
            num_scalar_prefetch=1,
            grid=(1,),
            in_specs=[VMEM, pl.BlockSpec(memory_space=pl.ANY)],
            out_specs=VMEM,
            scratch_shapes=[
                pltpu.VMEM((rows * TILE, width), bf16),
                pltpu.SemaphoreType.DMA((rows // group,)),
            ],
        ),
        out_shape=jax.ShapeDtypeStruct((rows, width), bf16),
        compiler_params=params(12),
        cost_estimate=pl.CostEstimate(
            flops=2_000_000_000, bytes_accessed=rows * TILE * width * 2, transcendentals=0
        ),
        name="lookup",
    )(block, pick, table)


def swap(array, axis, bit):
    size = lax.axis_size(axis)
    return lax.ppermute(array, axis, [(i, i ^ bit) for i in range(size)])


def sum_rows(array):
    size = lax.axis_size("mp")
    both = array + swap(array, "mp", 1)
    core = lax.axis_index("mp") % 2
    half = array.shape[0] // 2
    own = lax.dynamic_slice_in_dim(both, core * half, half, 0)
    bit = 2
    while bit < size:
        own = own + swap(own, "mp", bit)
        bit *= 2
    other = swap(own, "mp", 1)
    first = jnp.where(core == 0, own, other)
    second = jnp.where(core == 0, other, own)
    return jnp.concatenate([first, second], axis=0)


def project_kernel(embedded_ref, gain_ref, query_ref, key_ref, value_ref, out_ref, scaled):
    step = pl.program_id(0)
    tile = query_ref.shape[1]
    queries = tile * pl.num_programs(0)
    key_width = key_ref.shape[1]

    @pl.when(step == 0)
    def _():
        wide = embedded_ref[...].astype(f32)
        scaled[...] = (wide * gain_ref[...].astype(f32)).astype(bf16)
        squares = jnp.sum(wide * wide, axis=1, keepdims=True) * (LIFT / SHRINK)
        out_ref[:, queries + 2 * key_width :] = jnp.broadcast_to(squares, (wide.shape[0], LANES))
        out_ref[:, queries : queries + key_width] = LIFT * jnp.dot(
            scaled[...], key_ref[...], preferred_element_type=f32
        )
        out_ref[:, queries + key_width : queries + 2 * key_width] = LIFT * jnp.dot(
            scaled[...], value_ref[...], preferred_element_type=f32
        )

    start = pl.multiple_of(step * tile, tile)
    out_ref[:, pl.ds(start, tile)] = LIFT * jnp.dot(
        scaled[...], query_ref[...], preferred_element_type=f32
    )


def project(embedded, gain, query_weight, key_weight, value_weight):
    rows, depth = embedded.shape
    queries, key_width = query_weight.shape[1], key_weight.shape[1]
    tile = min(512, queries)
    total = queries + 2 * key_width + LANES
    whole = lambda i: (0, 0)
    return pl.pallas_call(
        project_kernel,
        grid=(queries // tile,),
        in_specs=[
            pl.BlockSpec((rows, depth), whole),
            pl.BlockSpec((1, depth), whole),
            pl.BlockSpec((depth, tile), lambda i: (0, i)),
            pl.BlockSpec((depth, key_width), whole),
            pl.BlockSpec((depth, key_width), whole),
        ],
        out_specs=pl.BlockSpec((rows, total), whole),
        out_shape=jax.ShapeDtypeStruct((rows, total), f32),
        scratch_shapes=[pltpu.VMEM((rows, depth), bf16)],
        compiler_params=params(20),
        cost_estimate=pl.CostEstimate(
            flops=2 * rows * depth * (queries + 2 * key_width),
            bytes_accessed=2 * depth * (rows + queries) + 4 * rows * total,
            transcendentals=0,
        ),
        name="project",
    )(embedded, gain[None, :], query_weight, key_weight, value_weight)


def finish_kernel(width, rotated, sums_ref, cos_ref, sin_ref, out_ref):
    split = sums_ref.shape[1] - LANES
    squares = sums_ref[:, split:] * (SHRINK / LIFT)
    inverse = 1.0 / jnp.sqrt(squares / width + epsilon)
    for start in range(0, split, HEAD_DIM):
        head = sums_ref[:, start : start + HEAD_DIM] * (1.0 / LIFT) * inverse
        if start < rotated:
            head = head * cos_ref[...] + pltpu.roll(head, HEAD_DIM // 2, 1) * sin_ref[...]
        out_ref[:, start : start + HEAD_DIM] = head.astype(bf16)


def finish(sums, cosine, sine, width, rotated):
    rows, total = sums.shape
    return pl.pallas_call(
        functools.partial(finish_kernel, width, rotated),
        in_specs=[VMEM] * 3,
        out_specs=VMEM,
        out_shape=jax.ShapeDtypeStruct((rows, total - LANES), bf16),
        compiler_params=params(8),
        cost_estimate=pl.CostEstimate(
            flops=1_000_000, bytes_accessed=8 * rows * total, transcendentals=0
        ),
        name="finish",
    )(sums, cosine, sine)


def visit_kernel(heads, key_heads, beams, scalars, rows_ref, parent_ref, keys_ref, values_ref, out_ref, fresh_ref):
    for n in range(keys_ref.shape[0]):
        own = slice(n * beams, (n + 1) * beams)
        attend(
            heads,
            key_heads,
            scalars,
            rows_ref[own, :],
            parent_ref[own, :],
            keys_ref[n],
            values_ref[n],
            out_ref.at[own, :],
            fresh_ref.at[n],
        )


def attend(heads, key_heads, scalars, rows, parents, keys, values, out_ref, fresh_ref):
    beams = rows.shape[0]
    groups = heads // key_heads
    query_width, key_width = heads * HEAD_DIM, key_heads * HEAD_DIM
    scale = HEAD_DIM ** (-0.5)
    arrived = rows.astype(f32)
    per_head = [arrived[:, h * HEAD_DIM : (h + 1) * HEAD_DIM] for h in range(heads)]
    own_keys = [
        arrived[:, query_width + k * HEAD_DIM : query_width + (k + 1) * HEAD_DIM]
        for k in range(key_heads)
    ]
    own_values = [
        arrived[:, query_width + key_width + k * HEAD_DIM : query_width + key_width + (k + 1) * HEAD_DIM]
        for k in range(key_heads)
    ]
    queries = jnp.concatenate(per_head, axis=0)
    key_rows = jnp.concatenate([own_keys[h // groups] for h in range(heads)], axis=0)
    value_rows = jnp.concatenate([own_values[h // groups] for h in range(heads)], axis=0)
    block = groups * beams
    zero = jnp.zeros((block, HEAD_DIM), f32)
    wide = jnp.concatenate(
        [
            jnp.concatenate(
                [queries[k * block : (k + 1) * block] if n == k else zero for n in range(key_heads)],
                axis=1,
            )
            for k in range(key_heads)
        ],
        axis=0,
    ).astype(bf16)
    scores = (
        lax.dot_general(wide, keys, (((1,), (1,)), ((), ())), preferred_element_type=f32)
        * scale
    )
    own = jnp.sum(queries * key_rows, axis=1, keepdims=True) * scale
    ceiling = jnp.maximum(jnp.max(scores, axis=1, keepdims=True), own)
    weights = jnp.exp(scores - ceiling)
    own_weight = jnp.exp(own - ceiling)
    share = 1.0 / (jnp.sum(weights, axis=1, keepdims=True) + own_weight)
    shares = (weights * share).astype(bf16)
    own_share = (own_weight * share).astype(bf16).astype(f32)
    mixed = jnp.dot(shares, values, preferred_element_type=f32)
    mixed = jnp.concatenate(
        [
            mixed[k * block : (k + 1) * block, k * HEAD_DIM : (k + 1) * HEAD_DIM]
            for k in range(key_heads)
        ],
        axis=0,
    )
    mixed = mixed + own_share * value_rows
    here = parents == scalars[2]
    for h in range(heads):
        out_ref[:, h * HEAD_DIM : (h + 1) * HEAD_DIM] = jnp.where(
            here, mixed[h * beams : (h + 1) * beams], per_head[h]
        ).astype(bf16)
    rest = arrived[:, query_width:]
    out_ref[:, query_width:] = rest.astype(bf16)
    beam = lax.broadcasted_iota(jnp.int32, rest.shape, 0)
    fresh_ref[...] = jnp.sum(jnp.where(beam == scalars[3], rest, 0.0), axis=0, keepdims=True).astype(bf16)


def visit(scalars, rows, parent_column, cache_keys, cache_values, heads, key_heads, beams):
    count, width = rows.shape
    requests = count // beams
    _, length, cache_width = cache_keys.shape
    at_once = min(2, requests)
    cached = pl.BlockSpec((at_once, length, cache_width), lambda t, s: (s[1] // at_once + t, 0, 0))
    return pl.pallas_call(
        functools.partial(visit_kernel, heads, key_heads, beams),
        grid_spec=pltpu.PrefetchScalarGridSpec(
            num_scalar_prefetch=1,
            grid=(requests // at_once,),
            in_specs=[
                pl.BlockSpec((at_once * beams, width), lambda t, s: (t, 0)),
                pl.BlockSpec((at_once * beams, 1), lambda t, s: (s[0] // at_once + t, 0)),
                cached,
                cached,
            ],
            out_specs=[
                pl.BlockSpec((at_once * beams, width), lambda t, s: (t, 0)),
                pl.BlockSpec((at_once, 1, 2 * cache_width), lambda t, s: (t, 0, 0)),
            ],
        ),
        out_shape=[
            jax.ShapeDtypeStruct((count, width), bf16),
            jax.ShapeDtypeStruct((requests, 1, 2 * cache_width), bf16),
        ],
        compiler_params=params(VISIT_MIB),
        cost_estimate=pl.CostEstimate(
            flops=8 * count * heads * length * HEAD_DIM,
            bytes_accessed=4 * requests * length * cache_width,
            transcendentals=count * heads * length,
        ),
        name="visit",
    )(scalars, rows, parent_column, cache_keys, cache_values)


def body(
    token_ids,
    parents,
    embedding,
    norm_gain,
    query_weight,
    key_weight,
    value_weight,
    output_weight,
    cache_keys,
    cache_values,
):
    ring, parts = lax.axis_size("beam"), lax.axis_size("mp")
    beam_at, mp_at = lax.axis_index("beam"), lax.axis_index("mp")
    beams = parents.shape[1]
    requests = parents.shape[0] * ring
    count = token_ids.shape[0]
    rows = count * ring
    width = norm_gain.shape[0] * ring
    heads, key_heads = query_weight.shape[1] // HEAD_DIM, key_weight.shape[1] // HEAD_DIM
    query_width, key_width = heads * HEAD_DIM, key_heads * HEAD_DIM
    row_local, length = cache_keys.shape[:2]

    walk = cycle(ring)
    place = np.argsort(np.array(walk)).astype(np.int32)
    at = jnp.asarray(place)[beam_at]
    ahead = [(walk[i], walk[(i + 1) % ring]) for i in range(ring)]
    back = [(b, a) for a, b in ahead]
    ways = ((ahead, 1), (back, -1))
    block = rows // ring
    piece = block // 2
    piece_requests = piece // beams
    share = requests // ring
    far = ring // 2
    order = [far] + [sign * d for d in range(far - 1, 0, -1) for sign in (1, -1)] + [0]

    mine = jnp.concatenate([token_ids, parents.reshape(-1)])[None, :]
    slot = lax.broadcasted_iota(jnp.int32, (ring, 1), 0) == beam_at
    every = lax.psum(jnp.where(slot, mine, 0), "beam")
    ids = every[:, :count].reshape(beams, requests).T.reshape(ring, block)
    parent_column = every[:, count:].reshape(rows, 1)
    ids = ids[(at + np.array(order, np.int32)) % ring]

    parts_of = []
    for half in (ids[:far], ids[far:]):
        embedded = sum_rows(lookup(half.reshape(-1), embedding))
        parts_of.append(project(embedded, norm_gain, query_weight, key_weight, value_weight))
    local = {}
    for n, distance in enumerate(order):
        local[distance] = parts_of[n // far][n % far * block : (n % far + 1) * block]

    def chunk(way, sign, step):
        return (at - sign * step) % ring

    sums = [local[far][:piece].astype(f16), local[far][piece:].astype(f16)]
    for step in range(1, far + 1):
        received = [lax.ppermute(m, "beam", pairs).astype(f32) for m, (pairs, _) in zip(sums, ways)]
        if step == 1:
            zero = jnp.zeros_like(received[0])
            received = [
                jnp.concatenate([received[0], zero], axis=0),
                jnp.concatenate([zero, received[1]], axis=0),
            ]
        if step < far:
            sums = [
                (got + local[sign * (far - step)]).astype(f16) for got, (_, sign) in zip(received, ways)
            ]
    angles = length * rope_base ** (-(jnp.arange(HEAD_DIM // 2, dtype=f32) * 2.0 / HEAD_DIM))
    cosine = jnp.concatenate([jnp.cos(angles)] * 2)[None, :]
    sine = jnp.concatenate([-jnp.sin(angles), jnp.sin(angles)])[None, :]
    home = finish(
        received[0] + received[1] + local[0], cosine, sine, width, query_width + key_width
    )
    moving = [home[:piece], home[piece:]]

    first_row = beam_at * row_local
    parent_here, request_start = first_row // requests, first_row % requests
    fresh = [[], []]
    for step in range(ring):
        for way, (pairs, sign) in enumerate(ways):
            if step:
                moving[way] = lax.ppermute(moving[way], "beam", pairs)
            request = chunk(way, sign, step) * share + way * piece_requests
            inside = (request >= request_start) & (request < request_start + row_local)
            scalars = jnp.stack(
                [
                    request,
                    jnp.where(inside, request - request_start, 0),
                    jnp.where(inside, parent_here, -1),
                    parent_here,
                ]
            ).astype(jnp.int32)
            moving[way], kept = visit(
                scalars, moving[way], parent_column, cache_keys, cache_values, heads, key_heads, beams
            )
            fresh[way].append(kept.reshape(piece_requests, 2 * key_width))

    columns = output_weight.shape[1]
    bits = parts.bit_length() - 1
    part_beams = beams // parts

    def products(packages):
        return jnp.dot(
            jnp.concatenate(packages, axis=0), output_weight, preferred_element_type=f32
        ).reshape((len(packages),) + (2,) * bits + (part_beams * 2 * piece_requests, columns))

    def scattered(partial):
        for n in range(bits):
            axis = partial.ndim - 3
            own_bit = (mp_at >> n) & 1
            keep = lax.dynamic_index_in_dim(partial, own_bit, axis, keepdims=False)
            send = lax.dynamic_index_in_dim(partial, 1 - own_bit, axis, keepdims=False)
            partial = keep + swap(send.astype(bf16), "mp", 1 << n).astype(f32)
        return partial.astype(bf16).reshape(-1, columns)

    package = jnp.stack([m[:, :query_width] for m in moving])
    package = package.reshape(2, piece_requests, beams, query_width)
    package = jnp.transpose(package, (2, 0, 1, 3)).reshape(block, query_width)
    outs, summed = [products([package])], []
    going = [package, package]
    for step in range(1, far + 1):
        if step == far:
            going = [going[0][:piece], going[1][piece:]]
        going = [lax.ppermute(g, "beam", pairs) for g, (pairs, _) in zip(going, ways)]
        if step == far:
            outs.append(products([jnp.concatenate(going, axis=0)]))
        else:
            outs.append(products(going))
        if step in (far - 2, far):
            summed.append(scattered(jnp.concatenate(outs, axis=0)))
            outs = []
    summed = jnp.concatenate(summed, axis=0)

    size = summed.shape[0]
    target = lax.broadcasted_iota(jnp.int32, (size, 1), 0)
    beam_of, request_of = target // requests, target % requests
    chunk_of, way_of = request_of // share, request_of % share // piece_requests
    distance = (chunk_of - (1 - 2 * way_of) - at) % ring
    package_of = jnp.where(
        distance == 0, 0, jnp.where(distance < far, 2 * distance, 2 * (ring - distance) - 1)
    )
    source = ((package_of * part_beams + beam_of) * 2 + way_of) * piece_requests
    source = source + request_of % piece_requests
    arrange = (lax.broadcasted_iota(jnp.int32, (size, size), 1) == source).astype(bf16)
    attention_out = jnp.dot(arrange, summed, preferred_element_type=f32).astype(bf16)

    seen = jnp.stack([jnp.stack(f) for f in fresh]).reshape(2 * ring * piece_requests, 2 * key_width)
    local_request = request_start + lax.broadcasted_iota(jnp.int32, (row_local, 1), 0)
    chunk_of, way_of = local_request // share, local_request % share // piece_requests
    sign_of = 1 - 2 * way_of
    step_of = (sign_of * (at - chunk_of)) % ring
    source = (way_of * ring + step_of) * piece_requests + local_request % piece_requests
    arrange = (lax.broadcasted_iota(jnp.int32, (row_local, seen.shape[0]), 1) == source).astype(bf16)
    fresh_rows = jnp.dot(arrange, seen, preferred_element_type=f32).astype(bf16)
    return attention_out, fresh_rows[:, :key_width], fresh_rows[:, key_width:]


def solution(mesh):
    return jax.shard_map(
        body,
        mesh=mesh,
        in_specs=(
            P("beam"),
            P("beam", None, None),
            P("mp", "beam"),
            P("beam"),
            P("beam", "mp"),
            P("beam", "mp"),
            P("beam", "mp"),
            P("mp", "beam"),
            P("beam", None, "mp"),
            P("beam", None, "mp"),
        ),
        out_specs=(P("mp", "beam"), P("beam", "mp"), P("beam", "mp")),
        check_vma=False,
    )
```

```python
import functools

import jax
import jax.numpy as jnp
import numpy as np
from jax import lax
from jax.experimental import pallas as pl
from jax.experimental.pallas import tpu as pltpu
from jax.sharding import PartitionSpec as P

HEAD_DIM = 128
LANES = 128
TILE = 8
LIFT = 8.0
SHRINK = 64.0
VISIT_MIB = 48
epsilon = 1e-05
rope_base = 500000.0


f32 = jnp.float32
bf16 = jnp.bfloat16
f16 = jnp.float16
VMEM = pl.BlockSpec(memory_space=pltpu.VMEM)


def params(mib=48, **more):
    return pltpu.CompilerParams(vmem_limit_bytes=mib << 20, **more)


def cycle(count):
    width = 1 << ((count.bit_length() - 1) // 2)
    height = count // width
    if width == 1 or height % 2:
        return list(range(count))
    walk = []
    for z in range(height):
        ys = range(1, width) if z % 2 == 0 else range(width - 1, 0, -1)
        walk += [z * width + y for y in ys]
    return walk + [z * width for z in range(height - 1, -1, -1)]


def place(index, count):
    width = 1 << ((count.bit_length() - 1) // 2)
    height = count // width
    if width == 1 or height % 2:
        return index
    z, y = index // width, index % width
    out = z * (width - 1) + jnp.where(z % 2 == 0, y - 1, width - 1 - y)
    return jnp.where(y == 0, height * (width - 1) + height - 1 - z, out)


def resident(position, count):
    width = 1 << ((count.bit_length() - 1) // 2)
    height = count // width
    if width == 1 or height % 2:
        return position
    z = position // (width - 1)
    y = jnp.where(z % 2 == 0, 1 + position % (width - 1), width - 1 - position % (width - 1))
    returning = position >= height * (width - 1)
    z = jnp.where(returning, height - 1 - (position - height * (width - 1)), z)
    return z * width + jnp.where(returning, 0, y)


def lookup_kernel(group, block_ref, pick_ref, table_ref, out_ref, held, sems):
    rows = out_ref.shape[0]
    groups = rows // group
    held[...] = jnp.zeros_like(held)

    def copy(i, g):
        source = pl.multiple_of(jnp.maximum(block_ref[i], 0) * TILE, TILE)
        target = pl.multiple_of(i * TILE, TILE)
        return pltpu.make_async_copy(
            table_ref.at[pl.ds(source, TILE), :], held.at[pl.ds(target, TILE), :], sems.at[g]
        )

    def issue(g, _):
        for n in range(group):
            i = g * group + n

            @pl.when(block_ref[i] >= 0)
            def _():
                copy(i, g).start()

        return 0

    lax.fori_loop(0, groups, issue, 0)

    def pick(g, _):
        for n in range(group):
            i = g * group + n

            @pl.when(block_ref[i] >= 0)
            def _():
                copy(i, g).wait()

        span = pl.ds(pl.multiple_of(g * group * TILE, group * TILE), group * TILE)
        own = pl.ds(pl.multiple_of(g * group, group), group)
        wanted = pick_ref[own, :]
        column = lax.broadcasted_iota(jnp.int32, (group, group * TILE), 1)
        row = lax.broadcasted_iota(jnp.int32, (group, group * TILE), 0)
        chosen = (column - row * TILE == wanted).astype(f32).astype(bf16)
        out_ref[own, :] = jnp.dot(chosen, held[span, :], preferred_element_type=f32).astype(bf16)
        return 0

    lax.fori_loop(0, groups, pick, 0)


def lookup(ids, table):
    rows, (vocab, width) = ids.shape[0], table.shape
    local = ids - lax.axis_index("mp") * vocab
    inside = (local >= 0) & (local < vocab)
    block = jnp.where(inside, local // TILE, -1)
    pick = jnp.where(inside, local % TILE, rows * TILE)[:, None]
    group = 32
    return pl.pallas_call(
        functools.partial(lookup_kernel, group),
        grid_spec=pltpu.PrefetchScalarGridSpec(
            num_scalar_prefetch=1,
            grid=(1,),
            in_specs=[VMEM, pl.BlockSpec(memory_space=pl.ANY)],
            out_specs=VMEM,
            scratch_shapes=[
                pltpu.VMEM((rows * TILE, width), bf16),
                pltpu.SemaphoreType.DMA((rows // group,)),
            ],
        ),
        out_shape=jax.ShapeDtypeStruct((rows, width), bf16),
        compiler_params=params(12),
        cost_estimate=pl.CostEstimate(
            flops=2_000_000_000, bytes_accessed=rows * TILE * width * 2, transcendentals=0
        ),
        name="lookup",
    )(block, pick, table)


def swap(array, axis, bit):
    size = lax.axis_size(axis)
    return lax.ppermute(array, axis, [(i, i ^ bit) for i in range(size)])


def sum_rows(array):
    size = lax.axis_size("mp")
    both = array + swap(array, "mp", 1)
    core = lax.axis_index("mp") % 2
    half = array.shape[0] // 2
    own = lax.dynamic_slice_in_dim(both, core * half, half, 0)
    bit = 2
    while bit < size:
        own = own + swap(own, "mp", bit)
        bit *= 2
    other = swap(own, "mp", 1)
    first = jnp.where(core == 0, own, other)
    second = jnp.where(core == 0, other, own)
    return jnp.concatenate([first, second], axis=0)


def project_kernel(embedded_ref, gain_ref, query_ref, key_ref, value_ref, out_ref, scaled):
    step = pl.program_id(0)
    tile = query_ref.shape[1]
    queries = tile * pl.num_programs(0)
    key_width = key_ref.shape[1]

    @pl.when(step == 0)
    def _():
        wide = embedded_ref[...].astype(f32)
        scaled[...] = (wide * gain_ref[...].astype(f32)).astype(bf16)
        squares = jnp.sum(wide * wide, axis=1, keepdims=True) * (LIFT / SHRINK)
        out_ref[:, queries + 2 * key_width :] = jnp.broadcast_to(squares, (wide.shape[0], LANES))
        out_ref[:, queries : queries + key_width] = LIFT * jnp.dot(
            scaled[...], key_ref[...], preferred_element_type=f32
        )
        out_ref[:, queries + key_width : queries + 2 * key_width] = LIFT * jnp.dot(
            scaled[...], value_ref[...], preferred_element_type=f32
        )

    start = pl.multiple_of(step * tile, tile)
    out_ref[:, pl.ds(start, tile)] = LIFT * jnp.dot(
        scaled[...], query_ref[...], preferred_element_type=f32
    )


def project(embedded, gain, query_weight, key_weight, value_weight):
    rows, depth = embedded.shape
    queries, key_width = query_weight.shape[1], key_weight.shape[1]
    tile = min(512, queries)
    total = queries + 2 * key_width + LANES
    whole = lambda i: (0, 0)
    return pl.pallas_call(
        project_kernel,
        grid=(queries // tile,),
        in_specs=[
            pl.BlockSpec((rows, depth), whole),
            pl.BlockSpec((1, depth), whole),
            pl.BlockSpec((depth, tile), lambda i: (0, i)),
            pl.BlockSpec((depth, key_width), whole),
            pl.BlockSpec((depth, key_width), whole),
        ],
        out_specs=pl.BlockSpec((rows, total), whole),
        out_shape=jax.ShapeDtypeStruct((rows, total), f32),
        scratch_shapes=[pltpu.VMEM((rows, depth), bf16)],
        compiler_params=params(20),
        cost_estimate=pl.CostEstimate(
            flops=2 * rows * depth * (queries + 2 * key_width),
            bytes_accessed=2 * depth * (rows + queries) + 4 * rows * total,
            transcendentals=0,
        ),
        name="project",
    )(embedded, gain[None, :], query_weight, key_weight, value_weight)


def finish_kernel(width, rotated, sums_ref, cos_ref, sin_ref, parent_ref, out_ref):
    split = sums_ref.shape[1] - LANES
    squares = sums_ref[:, split:] * (SHRINK / LIFT)
    inverse = 1.0 / jnp.sqrt(squares / width + epsilon)
    for start in range(0, split, HEAD_DIM):
        head = sums_ref[:, start : start + HEAD_DIM] * (1.0 / LIFT) * inverse
        if start < rotated:
            head = head * cos_ref[...] + pltpu.roll(head, HEAD_DIM // 2, 1) * sin_ref[...]
        out_ref[:, start : start + HEAD_DIM] = head.astype(bf16)
    named = parent_ref[...].astype(f32)
    out_ref[:, split:] = jnp.broadcast_to(named, (named.shape[0], LANES)).astype(bf16)


def finish(sums, cosine, sine, parents, width, rotated):
    rows, total = sums.shape
    return pl.pallas_call(
        functools.partial(finish_kernel, width, rotated),
        in_specs=[VMEM] * 4,
        out_specs=VMEM,
        out_shape=jax.ShapeDtypeStruct((rows, total), bf16),
        compiler_params=params(8),
        cost_estimate=pl.CostEstimate(
            flops=1_000_000, bytes_accessed=8 * rows * total, transcendentals=0
        ),
        name="finish",
    )(sums, cosine, sine, parents)


def visit_kernel(
    heads,
    key_heads,
    beams,
    entry,
    scalars,
    moving_ref,
    keys_ref,
    values_ref,
    out_ref,
    fresh_ref,
    rows_ref,
    keys,
    values,
    sems,
    rows_sem,
):
    requests = keys.shape[0]
    first, device, beam = scalars[entry], scalars[entry + 1], scalars[entry + 2]
    arriving = pltpu.make_async_copy(moving_ref, rows_ref, rows_sem)
    arriving.start()
    copies = []
    for n in range(requests):
        pair = (
            pltpu.make_async_copy(keys_ref.at[first + n], keys.at[n], sems.at[n, 0]),
            pltpu.make_async_copy(values_ref.at[first + n], values.at[n], sems.at[n, 1]),
        )
        for copy in pair:
            copy.start()
        copies.append(pair)
    arriving.wait()
    at_once = min(2, requests)
    for start in range(0, requests, at_once):
        for pair in copies[start : start + at_once]:
            for copy in pair:
                copy.wait()
        for n in range(start, start + at_once):
            own = slice(n * beams, (n + 1) * beams)
            attend(
                heads,
                key_heads,
                device,
                beam,
                rows_ref[own, :],
                keys[n],
                values[n],
                out_ref.at[own, :],
                fresh_ref.at[n],
            )


def attend(heads, key_heads, device, beam, rows, keys, values, out_ref, fresh_ref):
    beams = rows.shape[0]
    groups = heads // key_heads
    query_width, key_width = heads * HEAD_DIM, key_heads * HEAD_DIM
    rest_end = query_width + 2 * key_width
    scale = HEAD_DIM ** (-0.5)
    arrived = rows.astype(f32)
    per_head = [arrived[:, h * HEAD_DIM : (h + 1) * HEAD_DIM] for h in range(heads)]
    own_keys = [
        arrived[:, query_width + k * HEAD_DIM : query_width + (k + 1) * HEAD_DIM]
        for k in range(key_heads)
    ]
    own_values = [
        arrived[:, query_width + key_width + k * HEAD_DIM : query_width + key_width + (k + 1) * HEAD_DIM]
        for k in range(key_heads)
    ]
    queries = jnp.concatenate(per_head, axis=0)
    key_rows = jnp.concatenate([own_keys[h // groups] for h in range(heads)], axis=0)
    value_rows = jnp.concatenate([own_values[h // groups] for h in range(heads)], axis=0)
    block = groups * beams
    zero = jnp.zeros((block, HEAD_DIM), f32)
    wide = jnp.concatenate(
        [
            jnp.concatenate(
                [queries[k * block : (k + 1) * block] if n == k else zero for n in range(key_heads)],
                axis=1,
            )
            for k in range(key_heads)
        ],
        axis=0,
    ).astype(bf16)
    scores = (
        lax.dot_general(wide, keys, (((1,), (1,)), ((), ())), preferred_element_type=f32)
        * scale
    )
    own = jnp.sum(queries * key_rows, axis=1, keepdims=True) * scale
    ceiling = jnp.maximum(jnp.max(scores, axis=1, keepdims=True), own)
    weights = jnp.exp(scores - ceiling)
    own_weight = jnp.exp(own - ceiling)
    share = 1.0 / (jnp.sum(weights, axis=1, keepdims=True) + own_weight)
    shares = (weights * share).astype(bf16)
    own_share = (own_weight * share).astype(bf16).astype(f32)
    mixed = jnp.dot(shares, values, preferred_element_type=f32)
    mixed = jnp.concatenate(
        [
            mixed[k * block : (k + 1) * block, k * HEAD_DIM : (k + 1) * HEAD_DIM]
            for k in range(key_heads)
        ],
        axis=0,
    )
    mixed = mixed + own_share * value_rows
    here = arrived[:, rest_end : rest_end + 1] == device.astype(f32)
    for h in range(heads):
        out_ref[:, h * HEAD_DIM : (h + 1) * HEAD_DIM] = jnp.where(
            here, mixed[h * beams : (h + 1) * beams], per_head[h]
        ).astype(bf16)
    out_ref[:, query_width:] = rows[:, query_width:]
    rest = arrived[:, query_width:rest_end]
    beam_row = lax.broadcasted_iota(jnp.int32, rest.shape, 0)
    fresh_ref[...] = jnp.sum(jnp.where(beam_row == beam, rest, 0.0), axis=0, keepdims=True).astype(bf16)


def visit(entry, scalars, rows, cache_keys, cache_values, heads, key_heads, beams):
    count, width = rows.shape
    requests = count // beams
    _, length, cache_width = cache_keys.shape
    here = pl.BlockSpec((count, width), lambda t, s: (0, 0))
    outside = pl.BlockSpec(memory_space=pltpu.HBM)
    return pl.pallas_call(
        functools.partial(visit_kernel, heads, key_heads, beams, entry),
        grid_spec=pltpu.PrefetchScalarGridSpec(
            num_scalar_prefetch=1,
            grid=(1,),
            in_specs=[
                pl.BlockSpec(memory_space=pl.ANY),
                outside,
                outside,
            ],
            out_specs=[
                here,
                pl.BlockSpec((requests, 1, 2 * cache_width), lambda t, s: (0, 0, 0)),
            ],
            scratch_shapes=[
                pltpu.VMEM((count, width), bf16),
                pltpu.VMEM((requests, length, cache_width), bf16),
                pltpu.VMEM((requests, length, cache_width), bf16),
                pltpu.SemaphoreType.DMA((requests, 2)),
                pltpu.SemaphoreType.DMA(()),
            ],
        ),
        out_shape=[
            jax.ShapeDtypeStruct((count, width), bf16),
            jax.ShapeDtypeStruct((requests, 1, 2 * cache_width), bf16),
        ],
        compiler_params=params(VISIT_MIB),
        cost_estimate=pl.CostEstimate(
            flops=8 * count * heads * length * HEAD_DIM,
            bytes_accessed=4 * requests * length * cache_width,
            transcendentals=count * heads * length,
        ),
        name="visit",
    )(scalars, rows, cache_keys, cache_values)


def collect_kernel(scalars, *refs):
    pieces, out_ref = refs[:-1], refs[-1]
    for n, piece in enumerate(pieces):
        for row in range(piece.shape[0]):
            out_ref[scalars[4 * n + 3] + row] = piece[row]


def collect(scalars, pieces):
    count, _, width = pieces[0].shape
    return pl.pallas_call(
        collect_kernel,
        grid_spec=pltpu.PrefetchScalarGridSpec(
            num_scalar_prefetch=1,
            grid=(1,),
            in_specs=[VMEM] * len(pieces),
            out_specs=VMEM,
        ),
        out_shape=jax.ShapeDtypeStruct((count * len(pieces), 1, width), bf16),
        compiler_params=params(8),
        cost_estimate=pl.CostEstimate(flops=1_000_000, bytes_accessed=0, transcendentals=0),
        name="collect",
    )(scalars, *pieces)


def body(
    token_ids,
    parents,
    embedding,
    norm_gain,
    query_weight,
    key_weight,
    value_weight,
    output_weight,
    cache_keys,
    cache_values,
):
    ring, parts = lax.axis_size("beam"), lax.axis_size("mp")
    beam_at, mp_at = lax.axis_index("beam"), lax.axis_index("mp")
    beams = parents.shape[1]
    requests = parents.shape[0] * ring
    count = token_ids.shape[0]
    rows = count * ring
    width = norm_gain.shape[0] * ring
    heads, key_heads = query_weight.shape[1] // HEAD_DIM, key_weight.shape[1] // HEAD_DIM
    query_width, key_width = heads * HEAD_DIM, key_heads * HEAD_DIM
    row_local, length = cache_keys.shape[:2]

    walk = cycle(ring)
    at = place(beam_at, ring)
    ahead = [(walk[i], walk[(i + 1) % ring]) for i in range(ring)]
    back = [(b, a) for a, b in ahead]
    ways = ((ahead, 1), (back, -1))
    block = rows // ring
    piece = block // 2
    piece_requests = piece // beams
    share = requests // ring
    far = ring // 2
    order = [far] + [sign * d for d in range(far - 1, 0, -1) for sign in (1, -1)] + [0]

    slot = jnp.arange(rows, dtype=jnp.int32) // count == beam_at
    ids = lax.psum(jnp.where(slot, jnp.tile(token_ids, ring), 0), "beam")
    parents, ids = lax.optimization_barrier((parents, ids))
    ids = ids.reshape(beams, requests).T.reshape(ring, block)
    ids = ids[resident((at + jnp.asarray(order, jnp.int32)) % ring, ring)]

    parts_of = []
    for half in (ids[:far], ids[far:]):
        embedded = sum_rows(lookup(half.reshape(-1), embedding))
        parts_of.append(project(embedded, norm_gain, query_weight, key_weight, value_weight))
    local = {}
    for n, distance in enumerate(order):
        local[distance] = parts_of[n // far][n % far * block : (n % far + 1) * block]

    sums = [local[far][:piece].astype(f16), local[far][piece:].astype(f16)]
    for step in range(1, far + 1):
        received = [lax.ppermute(m, "beam", pairs).astype(f32) for m, (pairs, _) in zip(sums, ways)]
        if step == 1:
            zero = jnp.zeros_like(received[0])
            received = [
                jnp.concatenate([received[0], zero], axis=0),
                jnp.concatenate([zero, received[1]], axis=0),
            ]
        if step < far:
            sums = [
                (got + local[sign * (far - step)]).astype(f16) for got, (_, sign) in zip(received, ways)
            ]
    angles = length * rope_base ** (-(jnp.arange(HEAD_DIM // 2, dtype=f32) * 2.0 / HEAD_DIM))
    cosine = jnp.concatenate([jnp.cos(angles)] * 2)[None, :]
    sine = jnp.concatenate([-jnp.sin(angles), jnp.sin(angles)])[None, :]
    home = finish(
        received[0] + received[1] + local[0],
        cosine,
        sine,
        parents.reshape(block, 1),
        width,
        query_width + key_width,
    )
    moving = [home[:piece], home[piece:]]

    first_row = beam_at * row_local
    parent_here, request_start = first_row // requests, first_row % requests
    held = jnp.arange(2 * ring, dtype=jnp.int32)
    way_of = held % 2
    chunk_of = resident((at - (1 - 2 * way_of) * (held // 2)) % ring, ring)
    request = chunk_of * share + way_of * piece_requests
    inside = (request >= request_start) & (request < request_start + row_local)
    scalars = jnp.stack(
        [
            jnp.where(inside, request - request_start, 0),
            jnp.where(inside, parent_here, -1),
            jnp.full_like(held, parent_here),
            request,
        ],
        axis=1,
    ).reshape(-1)
    fresh = []
    for step in range(ring):
        for way, (pairs, sign) in enumerate(ways):
            if step:
                moving[way] = lax.ppermute(moving[way], "beam", pairs)
            moving[way], kept = visit(
                4 * (2 * step + way),
                scalars,
                moving[way],
                cache_keys,
                cache_values,
                heads,
                key_heads,
                beams,
            )
            fresh.append(kept)

    columns = output_weight.shape[1]
    bits = parts.bit_length() - 1
    part_beams = beams // parts

    def products(packages):
        return jnp.dot(
            jnp.concatenate(packages, axis=0), output_weight, preferred_element_type=f32
        ).reshape((len(packages),) + (2,) * bits + (part_beams * 2 * piece_requests, columns))

    def scattered(partial):
        for n in range(bits):
            axis = partial.ndim - 3
            own_bit = (mp_at >> n) & 1
            keep = lax.dynamic_index_in_dim(partial, own_bit, axis, keepdims=False)
            send = lax.dynamic_index_in_dim(partial, 1 - own_bit, axis, keepdims=False)
            partial = keep + swap(send.astype(bf16), "mp", 1 << n).astype(f32)
        return partial.astype(bf16).reshape(-1, columns)

    package = jnp.stack([m[:, :query_width] for m in moving])
    package = package.reshape(2, piece_requests, beams, query_width)
    package = jnp.transpose(package, (2, 0, 1, 3)).reshape(block, query_width)
    outs, summed = [products([package])], []
    going = [package, package]
    for step in range(1, far + 1):
        if step == far:
            going = [going[0][:piece], going[1][piece:]]
        going = [lax.ppermute(g, "beam", pairs) for g, (pairs, _) in zip(going, ways)]
        if step == far:
            outs.append(products([jnp.concatenate(going, axis=0)]))
        else:
            outs.append(products(going))
        if step in (far - 2, far):
            summed.append(scattered(jnp.concatenate(outs, axis=0)))
            outs = []
    summed = jnp.concatenate(summed, axis=0)

    size = summed.shape[0]
    target = lax.broadcasted_iota(jnp.int32, (size, 1), 0)
    beam_of, request_of = target // requests, target % requests
    chunk_of, way_of = request_of // share, request_of % share // piece_requests
    distance = (place(chunk_of, ring) - (1 - 2 * way_of) - at) % ring
    package_of = jnp.where(
        distance == 0, 0, jnp.where(distance < far, 2 * distance, 2 * (ring - distance) - 1)
    )
    source = ((package_of * part_beams + beam_of) * 2 + way_of) * piece_requests
    source = source + request_of % piece_requests
    arrange = (lax.broadcasted_iota(jnp.int32, (size, size), 1) == source).astype(bf16)
    attention_out = jnp.dot(arrange, summed, preferred_element_type=f32).astype(bf16)

    fresh_rows = collect(scalars, fresh).reshape(requests, 2 * key_width)
    fresh_rows = lax.dynamic_slice_in_dim(fresh_rows, request_start, row_local, 0)
    return attention_out, fresh_rows[:, :key_width], fresh_rows[:, key_width:]


def solution(mesh):
    return jax.shard_map(
        body,
        mesh=mesh,
        in_specs=(
            P("beam"),
            P("beam", None, None),
            P("mp", "beam"),
            P("beam"),
            P("beam", "mp"),
            P("beam", "mp"),
            P("beam", "mp"),
            P("mp", "beam"),
            P("beam", None, "mp"),
            P("beam", None, "mp"),
        ),
        out_specs=(P("mp", "beam"), P("beam", "mp"), P("beam", "mp")),
        check_vma=False,
    )
```
